32 devices in a mesh: dp: 2 (over core), gx: 4 (over y, x), gy: 4 (over z).
Axes of the slice: x: 2, y: 2, z: 4, core: 2. Of those that a mesh axis runs over, the one named last changes fastest.
Arguments:
- volume: bfloat16 [2, 4, 8, 32, 128], P('dp', None, 'gx', 'gy'), may hold values from -6 to 6
- targets: float32 [2, 4], P('dp'), may hold values from -4 to 4
- conv1_w: bfloat16 [27, 128], replicated, may hold values from -0.625 to 0.625
- conv1_b: float32 [32], replicated, may hold values from -3 to 3
- conv2_w: bfloat16 [27, 2048], replicated, may hold values from -0.21875 to 0.21875
- conv2_b: float32 [64], replicated, may hold values from -3 to 3
- head_w: float32 [64, 4], replicated, may hold values from -2 to 2
- head_b: float32 [4], replicated, may hold values from -4 to 4
- dir1: float32 [27, 128], replicated, may hold values from -6 to 6
- dir2: float32 [27, 2048], replicated, may hold values from -1.2 to 1.2
- dir_head: float32 [64, 4], replicated, may hold values from -6 to 6
Outputs:
- next1: float32 [27, 128], replicated
- next2: float32 [27, 2048], replicated
- next_head: float32 [64, 4], replicated
- rayleigh: float32 [], replicated
- curvature_field: float32 [2, 32, 8, 32, 128], P('dp', None, 'gx', 'gy')
The draws below stay inside these ranges and needn't reach their ends.
All inputs are finite; a program needn't handle non-finite values.
Results may differ from the reference program's by a relative error of at most 0.0051.
Values may be sent and summed in bfloat16 or wider, within the bound.
A program may use at most 128 MiB of HBM per device.

```python
import jax
import jax.numpy as jnp
from jax import lax

C0 = 4
C1 = 32
C2 = 64
OUT = 4
BATCH = 2
NX = 8
NY = 32
NZ = 128


def block_scale(stream_key, extent, cuts, smallest, top_value):
    def one(dim, parts):
        draws = jax.random.uniform(jax.random.fold_in(jax.random.fold_in(stream_key, 6), dim), (parts,), jnp.float32, smallest / len(cuts), top_value / len(cuts))
        return jnp.repeat(jnp.exp(draws), extent[dim] // parts).reshape((-1,) + (1,) * (len(extent) - dim - 1))

    gain = one(*cuts[0])
    for cut in cuts[1:]:
        gain = gain * one(*cut)
    return gain


def gaussian(rng, extent, scale, reach, cuts=(), dtype=jnp.bfloat16):
    factor_of = block_scale(rng, extent, cuts, -0.22, 0.18) if cuts else 1.0
    entries = jax.random.normal(rng, extent, jnp.float32) * scale * factor_of
    return jnp.minimum(jnp.maximum(entries, -reach), reach).astype(dtype)


def setup_inputs(seed: int = 0) -> dict:
    keys = jax.random.split(jax.random.key(seed), 12)
    volume = gaussian(keys[0], (BATCH, C0, NX, NY, NZ), 1.0, 6.0, ((0, 2), (2, 4), (3, 4)))
    targets = gaussian(keys[1], (BATCH, OUT), 1.0, 4.0, ((0, 2),), jnp.float32)
    conv1_w = gaussian(keys[2], (27, C1 * C0), (27 * C0) ** -0.5, 0.625)
    conv1_b = gaussian(keys[3], (C1,), 0.5, 3.0, (), jnp.float32)
    conv2_w = gaussian(keys[4], (27, C2 * C1), (27 * C1) ** -0.5, 0.21875)
    conv2_b = gaussian(keys[5], (C2,), 0.5, 3.0, (), jnp.float32)
    head_w = gaussian(keys[6], (C2, OUT), (C2 // 8) ** -0.5, 2.0, (), jnp.float32)
    head_b = gaussian(keys[7], (OUT,), 1.0, 4.0, (), jnp.float32)
    dir1 = gaussian(keys[8], (27, C1 * C0), 1.0, 6.0, (), jnp.float32)
    dir2 = gaussian(keys[9], (27, C2 * C1), 0.2, 1.2, (), jnp.float32)
    dir_head = gaussian(keys[10], (C2, OUT), 1.0, 6.0, (), jnp.float32)
    return dict(volume=volume, targets=targets, conv1_w=conv1_w, conv1_b=conv1_b, conv2_w=conv2_w, conv2_b=conv2_b, head_w=head_w, head_b=head_b, dir1=dir1, dir2=dir2, dir_head=dir_head)


def silu_parts(z):
    s = jax.nn.sigmoid(z)
    return (z * s, s * (1.0 + z * (1.0 - s)), s * (1.0 - s) * (2.0 + z * (1.0 - 2.0 * s)))

def as_kernel(flat, outer, inner):
    return flat.reshape(3, 3, 3, outer, inner).transpose(3, 4, 0, 1, 2)

def as_flat(kernel):
    return kernel.transpose(2, 3, 4, 0, 1).reshape(27, kernel.shape[0] * kernel.shape[1])

def pad_plane(a):
    return jnp.pad(a, ((0, 0), (0, 0), (1, 1), (1, 1), (0, 0)))

def pad_depth(a):
    return jnp.pad(a, ((0, 0), (0, 0), (0, 0), (0, 0), (1, 1)))

def convolve(padded, kernel):
    return lax.conv_general_dilated(pad_depth(padded), kernel, (1, 1, 1), 'VALID', dimension_numbers=('NCDHW', 'OIDHW', 'NCDHW'), preferred_element_type=jnp.float32)

def flipped(kernel):
    return jnp.flip(kernel, (2, 3, 4)).transpose(1, 0, 2, 3, 4)

def correlate(padded, grads):
    wide = pad_depth(padded)
    sx, sy, sz = (grads.shape[2], grads.shape[3], grads.shape[4])
    pieces = []
    for a in range(3):
        for b in range(3):
            for c in range(3):
                window = wide[:, :, a:a + sx, b:b + sy, c:c + sz]
                pieces.append(jnp.einsum('bixyz,boxyz->oi', window, grads, preferred_element_type=jnp.float32))
    stacked = jnp.stack(pieces, axis=0)
    return stacked.reshape(27, grads.shape[1] * padded.shape[1])

def spread(vector):
    return vector[:, :, None, None, None]

def reference(volume, targets, conv1_w, conv1_b, conv2_w, conv2_b, head_w, head_b, dir1, dir2, dir_head):
    high = lax.Precision.HIGHEST
    weight1 = as_kernel(conv1_w, C1, C0)
    weight2 = as_kernel(conv2_w, C2, C1)
    kern1 = as_kernel(dir1.astype(jnp.bfloat16), C1, C0)
    kern2 = as_kernel(dir2.astype(jnp.bfloat16), C2, C1)
    padded_in = pad_plane(volume)
    z1 = convolve(padded_in, weight1) + conv1_b[None, :, None, None, None]
    t1 = convolve(padded_in, kern1)
    act1, slope1, bend1 = silu_parts(z1)
    a1 = act1.astype(jnp.bfloat16)
    ta1 = (slope1 * t1).astype(jnp.bfloat16)
    pa1 = pad_plane(a1)
    pta1 = pad_plane(ta1)
    z2 = convolve(pa1, weight2) + conv2_b[None, :, None, None, None]
    t2 = convolve(pta1, weight2) + convolve(pa1, kern2)
    act2, slope2, bend2 = silu_parts(z2)
    cells = z2.shape[2] * z2.shape[3] * z2.shape[4]
    pooled = lax.optimization_barrier(jnp.sum(act2, axis=(2, 3, 4))) / cells
    tpooled = lax.optimization_barrier(jnp.sum(slope2 * t2, axis=(2, 3, 4))) / cells
    batch = volume.shape[0]
    outputs = jnp.dot(pooled, head_w, precision=high) + head_b
    toutputs = jnp.dot(tpooled, head_w, precision=high) + jnp.dot(pooled, dir_head, precision=high)
    dy = (outputs - targets) / batch
    tdy = toutputs / batch
    hd = jnp.dot(tpooled.T, dy, precision=high) + jnp.dot(pooled.T, tdy, precision=high)
    dpool = jnp.dot(dy, head_w.T, precision=high) / cells
    tdpool = (jnp.dot(tdy, head_w.T, precision=high) + jnp.dot(dy, dir_head.T, precision=high)) / cells
    g2 = (slope2 * spread(dpool)).astype(jnp.bfloat16)
    tg2 = (bend2 * t2 * spread(dpool) + slope2 * spread(tdpool)).astype(jnp.bfloat16)
    h2 = correlate(pa1, tg2) + correlate(pta1, g2)
    pg2 = pad_plane(g2)
    da1 = convolve(pg2, flipped(weight2))
    tda1 = convolve(pad_plane(tg2), flipped(weight2)) + convolve(pg2, flipped(kern2))
    tg1 = (bend1 * t1 * da1 + slope1 * tda1).astype(jnp.bfloat16)
    h1 = correlate(padded_in, tg1)
    field = tda1 * cells
    quad = jnp.sum(dir1 * h1) + jnp.sum(dir2 * h2) + jnp.sum(dir_head * hd)
    length = jnp.sum(dir1 * dir1) + jnp.sum(dir2 * dir2) + jnp.sum(dir_head * dir_head)
    nrm = jnp.sqrt(jnp.sum(h1 * h1) + jnp.sum(h2 * h2) + jnp.sum(hd * hd) + 1e-06)
    return (h1 / nrm, h2 / nrm, hd / nrm, quad / length, field)
```

```python
import jax
import jax.numpy as jnp
from jax import lax
from jax.experimental import pallas as pl
from jax.experimental.pallas import tpu as pltpu
from jax.sharding import PartitionSpec as P

C0 = 4
C1 = 32
C2 = 64
ROWS = 16
F32 = jnp.float32
BF16 = jnp.bfloat16


def extended(cells, sides, width):
    for axis, dim in sides:
        count = lax.axis_size(axis)
        ends = count - 1
        head = lax.slice_in_dim(cells, 0, width, axis=dim)
        tail = lax.slice_in_dim(cells, cells.shape[dim] - width, cells.shape[dim], axis=dim)
        cells = jnp.concatenate(
            [
                lax.ppermute(tail, axis, [(i, (i + 1) % count) for i in range(ends)]),
                cells,
                lax.ppermute(head, axis, [((i + 1) % count, i) for i in range(ends)]),
            ],
            axis=dim,
        )
    return cells


def silu_parts(z):
    s = 1.0 / (1.0 + jnp.exp(-z))
    return (z * s, s * (1.0 + z * (1.0 - s)), s * (1.0 - s) * (2.0 + z * (1.0 - 2.0 * s)))


def window(ref, x, y, count):
    columns = []
    for k in range(count):
        parts = []
        for a in range(3):
            rows = ref[x + a, y + k : y + k + 3]
            parts.append(rows.reshape(rows.shape[0] * rows.shape[1], rows.shape[2]))
        columns.append(jnp.concatenate(parts, axis=0))
    return jnp.concatenate(columns, axis=1)


def lane_of(shape):
    return lax.broadcasted_iota(jnp.int32, shape, 1)


def from_left(u):
    return jnp.where(lane_of(u.shape) == 0, 0.0, pltpu.roll(u, 1, 1))


def from_right(u):
    last = u.shape[1] - 1
    return jnp.where(lane_of(u.shape) == last, 0.0, pltpu.roll(u, last, 1))


def gathered(y, n):
    return from_left(y[:n]) + y[n : 2 * n] + from_right(y[2 * n : 3 * n])


def forward_kernel(v_ref, l1_ref, b1_ref, l2_ref, b2_ref, pq_ref, a_ref, ta_ref, d_ref, pool_ref, tpool_ref):
    nx, ny, lanes = (pq_ref.shape[1], pq_ref.shape[2], pq_ref.shape[4])
    b1 = b1_ref[...]
    l1 = l1_ref[...]
    for x in range(nx + 2):
        for y in range(0, ny + 2, 2):
            res = jnp.dot(l1, window(v_ref, x, y, 2), preferred_element_type=F32)
            for k in range(2):
                part = res[:, k * lanes : (k + 1) * lanes]
                z1 = part[:C1] + b1
                t1 = part[C1:]
                mask = v_ref[x + 1, y + k + 1].astype(F32)[3 * C0 : 3 * C0 + 1]
                act, slope, bend = silu_parts(z1)
                a_ref[x, y + k] = (act * mask).astype(BF16)
                ta_ref[x, y + k] = (slope * t1 * mask).astype(BF16)
                if 1 <= x <= nx and 1 <= y + k <= ny:
                    d_ref[0, x - 1, y + k - 1] = slope.astype(BF16)
                    d_ref[1, x - 1, y + k - 1] = (bend * t1).astype(BF16)
    b2 = b2_ref[...]
    n = 3 * C2
    total = jnp.zeros((C2, lanes), F32)
    ttotal = jnp.zeros((C2, lanes), F32)
    for x in range(nx):
        for y in range(0, ny, 2):
            res = jnp.dot(l2_ref[...], window(a_ref, x, y, 2), preferred_element_type=F32)
            tres = res[n:] + jnp.dot(l2_ref[:n], window(ta_ref, x, y, 2), preferred_element_type=F32)
            for k in range(2):
                z2 = gathered(res[:n, k * lanes : (k + 1) * lanes], C2) + b2
                t2 = gathered(tres[:, k * lanes : (k + 1) * lanes], C2)
                act, slope, bend = silu_parts(z2)
                total = total + act
                ttotal = ttotal + slope * t2
                pq_ref[0, x, y + k] = slope.astype(BF16)
                pq_ref[1, x, y + k] = (bend * t2).astype(BF16)
    pool_ref[...] = jnp.sum(total, axis=1, keepdims=True)
    tpool_ref[...] = jnp.sum(ttotal, axis=1, keepdims=True)


NT = (((1,), (1,)), ((), ()))


def backward_kernel(
    cells, batch, pq_ref, a_ref, ta_ref, d_ref, v_ref, lb_ref, pool_ref, tpool_ref, targets_ref,
    head_w_ref, head_b_ref, dir_head_ref, h2_ref, h1_ref, hd_ref, field_ref, g_ref, tg_ref, t1_ref,
):
    nx, ny, lanes = (d_ref.shape[1], d_ref.shape[2], d_ref.shape[4])
    pooled = pool_ref[...] / cells
    tpooled = tpool_ref[...] / cells
    head_w = head_w_ref[...]
    dir_head = dir_head_ref[...]
    out = jnp.sum(pooled * head_w, axis=0, keepdims=True) + head_b_ref[...]
    tout = jnp.sum(tpooled * head_w + pooled * dir_head, axis=0, keepdims=True)
    dy = (out - targets_ref[...]) / batch
    tdy = tout / batch
    hd_ref[...] = tpooled * dy + pooled * tdy
    dpool = jnp.sum(dy * head_w, axis=1, keepdims=True) / cells
    tdpool = jnp.sum(tdy * head_w + dy * dir_head, axis=1, keepdims=True) / cells
    for x in range(nx + 2):
        for y in range(ny + 2):
            slope = pq_ref[0, x, y].astype(F32)
            bent = pq_ref[1, x, y].astype(F32)
            g_ref[x, y] = (slope * dpool).astype(BF16)
            tg_ref[x, y] = (bent * dpool + slope * tdpool).astype(BF16)

    def moved(ref, x, y):
        columns = []
        for k in range(2):
            u = ref[x + 1, y + k + 1].astype(F32)
            columns.append(jnp.concatenate([from_right(u), u, from_left(u)], axis=0).astype(BF16))
        return jnp.concatenate(columns, axis=1)

    h2 = jnp.zeros(h2_ref.shape, F32)
    for x in range(nx):
        for y in range(0, ny, 2):
            h2 = h2 + lax.dot_general(moved(tg_ref, x, y), window(a_ref, x, y, 2), NT, preferred_element_type=F32)
            h2 = h2 + lax.dot_general(moved(g_ref, x, y), window(ta_ref, x, y, 2), NT, preferred_element_type=F32)
    h2_ref[...] = h2
    n = 3 * C1
    h1 = jnp.zeros(h1_ref.shape, F32)
    for x in range(nx):
        for y in range(0, ny, 2):
            res = jnp.dot(lb_ref[...], window(g_ref, x, y, 2), preferred_element_type=F32)
            tres = res[n:] + jnp.dot(lb_ref[:n], window(tg_ref, x, y, 2), preferred_element_type=F32)
            grads = []
            for k in range(2):
                da = gathered(res[:n, k * lanes : (k + 1) * lanes], C1)
                tda = gathered(tres[:, k * lanes : (k + 1) * lanes], C1)
                field_ref[:, x, y + k, :] = tda * cells
                grads.append((d_ref[1, x, y + k].astype(F32) * da + d_ref[0, x, y + k].astype(F32) * tda).astype(BF16))
            h1 = h1 + lax.dot_general(
                jnp.concatenate(grads, axis=1), window(v_ref, x + 1, y + 1, 2), NT, preferred_element_type=F32
            )
    h1_ref[...] = h1


def vmem_call(kernel, shapes, scratch=()):
    return pl.pallas_call(
        kernel,
        out_shape=shapes,
        scratch_shapes=scratch,
        compiler_params=pltpu.CompilerParams(vmem_limit_bytes=48 * 1024 * 1024),
    )


def per_device(
    volume, targets, conv1_w, conv1_b, conv2_w, conv2_b, head_w, head_b, dir1, dir2, dir_head
):
    nx, ny, lanes = volume.shape[2:]
    cells = nx * lax.axis_size("gx") * ny * lax.axis_size("gy") * lanes
    batch = volume.shape[0] * lax.axis_size("dp")
    rows = volume[0].transpose(1, 2, 0, 3)
    wide = jnp.pad(rows, ((0, 0), (0, 0), (0, 0), (1, 1)))
    v = jnp.concatenate(
        [wide[..., :lanes], rows, wide[..., 2:], jnp.ones((nx, ny, 1, lanes), BF16), jnp.zeros((nx, ny, 3, lanes), BF16)],
        axis=2,
    )
    v = extended(v, (("gx", 0), ("gy", 1)), 2)
    first = jnp.stack((conv1_w, dir1.astype(BF16))).reshape(2, 9, 3, C1, C0)
    first = first.transpose(0, 3, 1, 2, 4).reshape(2 * C1, 9, 3 * C0)
    l1 = jnp.pad(first, ((0, 0), (0, 0), (0, ROWS - 3 * C0))).reshape(2 * C1, 9 * ROWS)
    second = jnp.stack((conv2_w, dir2.astype(BF16))).reshape(2, 9, 3, C2, C1)
    l2 = second.transpose(0, 2, 3, 1, 4).reshape(6 * C2, 9 * C1)
    lb = jnp.flip(second, (1, 2)).transpose(0, 2, 4, 1, 3).reshape(6 * C1, 9 * C2)
    shape = jax.ShapeDtypeStruct
    pq, a1, ta1, d, pool, tpool = vmem_call(
        forward_kernel,
        (
            shape((2, nx, ny, C2, lanes), BF16),
            shape((nx + 2, ny + 2, C1, lanes), BF16),
            shape((nx + 2, ny + 2, C1, lanes), BF16),
            shape((2, nx, ny, C1, lanes), BF16),
            shape((C2, 1), F32),
            shape((C2, 1), F32),
        ),
    )(v, l1, conv1_b[:, None], l2, conv2_b[:, None])
    pool, tpool = lax.psum((pool, tpool), ("gx", "gy"))
    pq = extended(pq, (("gx", 1), ("gy", 2)), 1)

    def backward(*refs):
        backward_kernel(cells, batch, *refs)

    h2, h1, hd, field = vmem_call(
        backward,
        (
            shape((3 * C2, 9 * C1), F32),
            shape((C1, 9 * ROWS), F32),
            shape((C2, head_w.shape[1]), F32),
            shape((C1, nx, ny, lanes), F32),
        ),
        (
            pltpu.VMEM((nx + 2, ny + 2, C2, lanes), BF16),
            pltpu.VMEM((nx + 2, ny + 2, C2, lanes), BF16),
            pltpu.VMEM((8, lanes), F32),
        ),
    )(pq, a1, ta1, d, v, lb, pool, tpool, targets, head_w, head_b[None], dir_head)
    leader = ((lax.axis_index("gx") == 0) & (lax.axis_index("gy") == 0)).astype(F32)
    h2, h1, hd = lax.psum((h2, h1, leader * hd), ("dp", "gx", "gy"))
    h2 = h2.reshape(3, C2, 9, C1).transpose(2, 0, 1, 3).reshape(27, C2 * C1)
    h1 = h1.reshape(C1, 9, ROWS)[:, :, : 3 * C0].reshape(C1, 27, C0).transpose(1, 0, 2).reshape(27, C1 * C0)
    quad = jnp.sum(dir1 * h1) + jnp.sum(dir2 * h2) + jnp.sum(dir_head * hd)
    length = jnp.sum(dir1 * dir1) + jnp.sum(dir2 * dir2) + jnp.sum(dir_head * dir_head)
    nrm = jnp.sqrt(jnp.sum(h1 * h1) + jnp.sum(h2 * h2) + jnp.sum(hd * hd) + 1e-06)
    return (h1 / nrm, h2 / nrm, hd / nrm, quad / length, field[None])


def solution(mesh):
    return jax.shard_map(
        per_device,
        mesh=mesh,
        in_specs=(P("dp", None, "gx", "gy", None), P("dp", None)) + (P(),) * 9,
        out_specs=(P(), P(), P(), P(), P("dp", None, "gx", "gy", None)),
        check_vma=False,
    )
```

```python
import jax
import jax.numpy as jnp
from jax import lax
from jax.experimental import pallas as pl
from jax.experimental.pallas import tpu as pltpu
from jax.sharding import PartitionSpec as P

C0 = 4
C1 = 32
C2 = 64
ROWS = 16
F32 = jnp.float32
BF16 = jnp.bfloat16


def extended(cells, sides, width):
    for axis, dim in sides:
        count = lax.axis_size(axis)
        ends = count - 1
        head = lax.slice_in_dim(cells, 0, width, axis=dim)
        tail = lax.slice_in_dim(cells, cells.shape[dim] - width, cells.shape[dim], axis=dim)
        cells = jnp.concatenate(
            [
                lax.ppermute(tail, axis, [(i, (i + 1) % count) for i in range(ends)]),
                cells,
                lax.ppermute(head, axis, [((i + 1) % count, i) for i in range(ends)]),
            ],
            axis=dim,
        )
    return cells


def swapped_sum(u, axis):
    count = lax.axis_size(axis)
    if count & (count - 1):
        return lax.psum(u, axis)
    step = 1
    while step < count:
        u = u + lax.ppermute(u, axis, [(i, i ^ step) for i in range(count)])
        step *= 2
    return u


def swapped(u, axis):
    return lax.ppermute(u, axis, [(0, 1), (1, 0)])


def total_sum(u):
    if lax.axis_size("dp") != 2:
        return lax.psum(u, ("dp", "gx", "gy"))
    half = u.shape[0] // 2
    me = lax.axis_index("dp")
    mine = lax.dynamic_slice_in_dim(u, me * half, half, 0)
    other = lax.dynamic_slice_in_dim(u, (1 - me) * half, half, 0)
    mine = mine + swapped(other, "dp")
    mine = swapped_sum(swapped_sum(mine, "gx"), "gy")
    other = swapped(mine, "dp")
    first = me == 0
    return jnp.concatenate([jnp.where(first, mine, other), jnp.where(first, other, mine)], axis=0)


def silu_parts(z):
    s = 1.0 / (1.0 + jnp.exp(-z))
    return (z * s, s * (1.0 + z * (1.0 - s)), s * (1.0 - s) * (2.0 + z * (1.0 - 2.0 * s)))


def window(ref, x, y, count):
    columns = []
    for k in range(count):
        parts = []
        for a in range(3):
            rows = ref[x + a, y + k : y + k + 3]
            parts.append(rows.reshape(rows.shape[0] * rows.shape[1], rows.shape[2]))
        columns.append(jnp.concatenate(parts, axis=0))
    return jnp.concatenate(columns, axis=1)


def lane_of(shape):
    return lax.broadcasted_iota(jnp.int32, shape, 1)


def from_left(u):
    return jnp.where(lane_of(u.shape) == 0, 0.0, pltpu.roll(u, 1, 1))


def from_right(u):
    last = u.shape[1] - 1
    return jnp.where(lane_of(u.shape) == last, 0.0, pltpu.roll(u, last, 1))


def gathered(y, n):
    return from_left(y[:n]) + y[n : 2 * n] + from_right(y[2 * n : 3 * n])


def forward_kernel(v_ref, l1_ref, b1_ref, l2_ref, b2_ref, pq_ref, a_ref, ta_ref, d_ref, pool_ref):
    nx, ny, lanes = (pq_ref.shape[1], pq_ref.shape[2], pq_ref.shape[4])
    b1 = b1_ref[...]
    l1 = l1_ref[...]
    for x in range(nx + 2):
        for y in range(0, ny + 2, 2):
            res = jnp.dot(l1, window(v_ref, x, y, 2), preferred_element_type=F32)
            for k in range(2):
                part = res[:, k * lanes : (k + 1) * lanes]
                z1 = part[:C1] + b1
                t1 = part[C1:]
                mask = v_ref[x + 1, y + k + 1].astype(F32)[3 * C0 : 3 * C0 + 1]
                act, slope, bend = silu_parts(z1)
                a_ref[x, y + k] = (act * mask).astype(BF16)
                ta_ref[x, y + k] = (slope * t1 * mask).astype(BF16)
                if 1 <= x <= nx and 1 <= y + k <= ny:
                    d_ref[0, x - 1, y + k - 1] = slope.astype(BF16)
                    d_ref[1, x - 1, y + k - 1] = (bend * t1).astype(BF16)
    b2 = b2_ref[...]
    n = 3 * C2
    total = jnp.zeros((C2, lanes), F32)
    ttotal = jnp.zeros((C2, lanes), F32)
    for x in range(nx):
        for y in range(0, ny, 2):
            res = jnp.dot(l2_ref[...], window(a_ref, x, y, 2), preferred_element_type=F32)
            tres = res[n:] + jnp.dot(l2_ref[:n], window(ta_ref, x, y, 2), preferred_element_type=F32)
            for k in range(2):
                z2 = gathered(res[:n, k * lanes : (k + 1) * lanes], C2) + b2
                t2 = gathered(tres[:, k * lanes : (k + 1) * lanes], C2)
                act, slope, bend = silu_parts(z2)
                total = total + act
                ttotal = ttotal + slope * t2
                pq_ref[0, x, y + k] = slope.astype(BF16)
                pq_ref[1, x, y + k] = (bend * t2).astype(BF16)
    both = (jnp.sum(total, axis=1, keepdims=True), jnp.sum(ttotal, axis=1, keepdims=True))
    pool_ref[...] = jnp.where(lane_of(pool_ref.shape) == 0, both[0], both[1])


NT = (((1,), (1,)), ((), ()))


def backward_kernel(
    cells, batch, pq_ref, a_ref, ta_ref, d_ref, v_ref, lb_ref, pool_ref, targets_ref,
    head_w_ref, head_b_ref, dir_head_ref, h_ref, hd_ref, field_ref, g_ref, tg_ref,
):
    nx, ny, lanes = (d_ref.shape[1], d_ref.shape[2], d_ref.shape[4])
    pooled = pool_ref[:, 0:1] / cells
    tpooled = pool_ref[:, 1:2] / cells
    head_w = head_w_ref[...]
    dir_head = dir_head_ref[...]
    out = jnp.sum(pooled * head_w, axis=0, keepdims=True) + head_b_ref[...]
    tout = jnp.sum(tpooled * head_w + pooled * dir_head, axis=0, keepdims=True)
    dy = (out - targets_ref[...]) / batch
    tdy = tout / batch
    hd_ref[...] = tpooled * dy + pooled * tdy
    dpool = jnp.sum(dy * head_w, axis=1, keepdims=True) / cells
    tdpool = jnp.sum(tdy * head_w + dy * dir_head, axis=1, keepdims=True) / cells
    for x in range(nx + 2):
        for y in range(ny + 2):
            slope = pq_ref[0, x, y].astype(F32)
            bent = pq_ref[1, x, y].astype(F32)
            g_ref[x, y] = (slope * dpool).astype(BF16)
            tg_ref[x, y] = (bent * dpool + slope * tdpool).astype(BF16)

    def moved(ref, x, y):
        columns = []
        for k in range(2):
            u = ref[x + 1, y + k + 1].astype(F32)
            columns.append(jnp.concatenate([from_right(u), u, from_left(u)], axis=0).astype(BF16))
        return jnp.concatenate(columns, axis=1)

    cut = 8 * C1
    most = jnp.zeros((3 * C2, cut), F32)
    rest = jnp.zeros((C1, 3 * C2), F32)
    for x in range(nx):
        for y in range(0, ny, 2):
            for grads, cells_ref in ((tg_ref, a_ref), (g_ref, ta_ref)):
                g = moved(grads, x, y)
                u = window(cells_ref, x, y, 2)
                most = most + lax.dot_general(g, u[:cut], NT, preferred_element_type=F32)
                rest = rest + lax.dot_general(u[cut:], g, NT, preferred_element_type=F32)
    top = 3 * C2
    h_ref[:top, :] = most
    h_ref[top:, :] = jnp.zeros((2 * C1, cut), F32)
    h_ref[top : top + C1, : 3 * C2] = rest
    n = 3 * C1
    h1 = jnp.zeros((C1, 9 * ROWS), F32)
    for x in range(nx):
        for y in range(0, ny, 2):
            res = jnp.dot(lb_ref[...], window(g_ref, x, y, 2), preferred_element_type=F32)
            tres = res[n:] + jnp.dot(lb_ref[:n], window(tg_ref, x, y, 2), preferred_element_type=F32)
            grads = []
            for k in range(2):
                da = gathered(res[:n, k * lanes : (k + 1) * lanes], C1)
                tda = gathered(tres[:, k * lanes : (k + 1) * lanes], C1)
                field_ref[:, x, y + k, :] = tda * cells
                grads.append((d_ref[1, x, y + k].astype(F32) * da + d_ref[0, x, y + k].astype(F32) * tda).astype(BF16))
            h1 = h1 + lax.dot_general(
                jnp.concatenate(grads, axis=1), window(v_ref, x + 1, y + 1, 2), NT, preferred_element_type=F32
            )
    h_ref[top + C1 :, : 9 * ROWS] = h1


def vmem_call(kernel, shapes, scratch=()):
    return pl.pallas_call(
        kernel,
        out_shape=shapes,
        scratch_shapes=scratch,
        compiler_params=pltpu.CompilerParams(vmem_limit_bytes=48 * 1024 * 1024),
    )


def per_device(
    volume, targets, conv1_w, conv1_b, conv2_w, conv2_b, head_w, head_b, dir1, dir2, dir_head
):
    nx, ny, lanes = volume.shape[2:]
    cells = nx * lax.axis_size("gx") * ny * lax.axis_size("gy") * lanes
    batch = volume.shape[0] * lax.axis_size("dp")
    rows = volume[0].transpose(1, 2, 0, 3)
    wide = jnp.pad(rows, ((0, 0), (0, 0), (0, 0), (1, 1)))
    v = jnp.concatenate(
        [wide[..., :lanes], rows, wide[..., 2:], jnp.ones((nx, ny, 1, lanes), BF16), jnp.zeros((nx, ny, 3, lanes), BF16)],
        axis=2,
    )
    v = extended(v, (("gx", 0), ("gy", 1)), 2)
    first = jnp.stack((conv1_w, dir1.astype(BF16))).reshape(2, 9, 3, C1, C0)
    first = first.transpose(0, 3, 1, 2, 4).reshape(2 * C1, 9, 3 * C0)
    l1 = jnp.pad(first, ((0, 0), (0, 0), (0, ROWS - 3 * C0))).reshape(2 * C1, 9 * ROWS)
    second = jnp.stack((conv2_w, dir2.astype(BF16))).reshape(2, 9, 3, C2, C1)
    l2 = second.transpose(0, 2, 3, 1, 4).reshape(6 * C2, 9 * C1)
    lb = jnp.flip(second, (1, 2)).transpose(0, 2, 4, 1, 3).reshape(6 * C1, 9 * C2)
    shape = jax.ShapeDtypeStruct
    pq, a1, ta1, d, pool = vmem_call(
        forward_kernel,
        (
            shape((2, nx, ny, C2, lanes), BF16),
            shape((nx + 2, ny + 2, C1, lanes), BF16),
            shape((nx + 2, ny + 2, C1, lanes), BF16),
            shape((2, nx, ny, C1, lanes), BF16),
            shape((C2, 2), F32),
        ),
    )(v, l1, conv1_b[:, None], l2, conv2_b[:, None])
    pool = swapped_sum(swapped_sum(pool, "gx"), "gy")
    pq = extended(pq, (("gx", 1), ("gy", 2)), 1)

    def backward(*refs):
        backward_kernel(cells, batch, *refs)

    h, hd, field = vmem_call(
        backward,
        (
            shape((3 * C2 + 2 * C1, 8 * C1), F32),
            shape((C2, head_w.shape[1]), F32),
            shape((C1, nx, ny, lanes), F32),
        ),
        (
            pltpu.VMEM((nx + 2, ny + 2, C2, lanes), BF16),
            pltpu.VMEM((nx + 2, ny + 2, C2, lanes), BF16),
        ),
    )(pq, a1, ta1, d, v, lb, pool, targets, head_w, head_b[None], dir_head)
    hd = swapped_sum(hd, "dp")
    h = total_sum(h)
    top = 3 * C2
    most = h[:top].reshape(3, C2, 8, C1).transpose(2, 0, 1, 3).reshape(24, C2 * C1)
    rest = h[top : top + C1, :top].reshape(C1, 3, C2).transpose(1, 2, 0).reshape(3, C2 * C1)
    h2 = jnp.concatenate([most, rest], axis=0)
    h1 = h[top + C1 :, : 9 * ROWS].reshape(C1, 9, ROWS)[:, :, : 3 * C0]
    h1 = h1.reshape(C1, 27, C0).transpose(1, 0, 2).reshape(27, C1 * C0)
    quad = jnp.sum(dir1 * h1) + jnp.sum(dir2 * h2) + jnp.sum(dir_head * hd)
    length = jnp.sum(dir1 * dir1) + jnp.sum(dir2 * dir2) + jnp.sum(dir_head * dir_head)
    nrm = jnp.sqrt(jnp.sum(h1 * h1) + jnp.sum(h2 * h2) + jnp.sum(hd * hd) + 1e-06)
    return (h1 / nrm, h2 / nrm, hd / nrm, quad / length, field[None])


def solution(mesh):
    return jax.shard_map(
        per_device,
        mesh=mesh,
        in_specs=(P("dp", None, "gx", "gy", None), P("dp", None)) + (P(),) * 9,
        out_specs=(P(), P(), P(), P(), P("dp", None, "gx", "gy", None)),
        check_vma=False,
    )
```
